32 devices in a mesh: dp: 16 (over z, x, core), tensor: 2 (over y).
Axes of the slice: x: 2, y: 2, z: 4, core: 2. Of those that a mesh axis runs over, the one named last changes fastest.
Arguments:
- query_rows: bfloat16 [6144, 5120], P('dp', 'tensor'), may hold values from -128 to 128
- key_rows: bfloat16 [6144, 5120], P('dp', 'tensor'), may hold values from -5 to 5
- value_rows: bfloat16 [6144, 5120], P('dp', 'tensor'), may hold values from -12 to 12
- action_mask: int32 [16, 384], P('dp'), may hold values from 0 to 1, as said below
- residual: bfloat16 [6144, 5120], P('dp', 'tensor'), may hold values from -100 to 100
- out_weight: bfloat16 [5120, 5120], P(None, 'tensor'), may hold values from -0.078125 to 0.078125
- norm_gain: float32 [5120], P('tensor'), may hold values from 0.1 to 1.9
- upstream: bfloat16 [6144, 5120], P('dp', 'tensor'), may hold values from -6 to 6
- residual_grad: bfloat16 [6144, 5120], P('dp', 'tensor'), may hold values from -2 to 2
Outputs:
- layer_out: bfloat16 [6144, 5120], P('dp', 'tensor')
- grad_residual: bfloat16 [6144, 5120], P('dp', 'tensor')
- grad_query: bfloat16 [6144, 5120], P('dp', 'tensor')
- grad_key: bfloat16 [6144, 5120], P('dp', 'tensor')
- grad_value: bfloat16 [6144, 5120], P('dp', 'tensor')
- grad_out_weight: float32 [5120, 5120], P('dp', 'tensor')
- grad_gain: float32 [5120], P('tensor')
The draws below stay inside these ranges and needn't reach their ends.
Inputs may be any that keep to these rules, and one draw needn't show every extreme that they name: `action_mask`: each row is a run of zeros followed by a run of ones; the ones number 1 to 192.
All inputs are finite; a program needn't handle non-finite values.
Results may differ from the reference program's by a relative error of at most 0.015.
Values may be sent and summed in bfloat16 or wider, within the bound.
A program may use at most 192 MiB of HBM per device.

```python
import jax
import jax.numpy as jnp
from jax import lax

D = 5120
HEADS = 40
HEAD_DIM = 128
LEN = 384
SEQS = 16
TOKENS = 6144


def attention_inputs(key):
    base_key = jax.random.fold_in(key, 17)
    key_query, key_key = jax.random.split(base_key, 2)
    shape = (SEQS, LEN, HEADS, HEAD_DIM)
    query_draw = jax.random.truncated_normal(key_query, -4.0, 4.0, shape, jnp.float32)
    key_draw = jax.random.truncated_normal(key_key, -4.0, 4.0, shape, jnp.float32)
    width = HEADS * HEAD_DIM
    return (query_draw.reshape(TOKENS, width), key_draw.reshape(TOKENS, width))


def draw_query_rows(key, part):
    return attention_inputs(key)[0].astype(jnp.bfloat16)


def draw_key_rows(key, part):
    return attention_inputs(key)[1].astype(jnp.bfloat16)


def draw_residual(key, part):
    key_base, key_rows = jax.random.split(jax.random.fold_in(key, 29), 2)
    columns = jnp.arange(D).astype(jnp.float32)
    column_scale = 10.0 ** (0.5 * columns / (D - 1))
    row_scale = jnp.exp(jax.random.uniform(key_rows, (TOKENS, 1), jnp.float32, jnp.log(0.5), jnp.log(5.0)))
    base = jax.random.truncated_normal(key_base, -5.0, 5.0, (TOKENS, D), jnp.float32)
    return (base * row_scale * column_scale[None, :]).astype(jnp.bfloat16)


def draw_action_mask(key, part):
    actions = jax.random.randint(jax.random.fold_in(key, 41), (SEQS,), 1, LEN // 2 + 1)
    position = jnp.arange(LEN)
    return (position[None, :] >= LEN - actions[:, None]).astype(jnp.int32)


def spiked(drawn, stream_key, source, target, parts, factor):
    def block_of(dim):
        return (jnp.arange(drawn.shape[dim]) // (drawn.shape[dim] // parts)).reshape((-1,) + (1,) * (drawn.ndim - 1 - dim))

    first = jax.random.permutation(stream_key, parts)[block_of(target)]
    far = (block_of(target) + parts // 2) % parts
    return jnp.where((block_of(source) == first) | (block_of(source) == far), factor * drawn, drawn)


def steps_of(rng, extent, shards, least, high):
    def one(dim, parts):
        heights = jax.random.uniform(jax.random.fold_in(jax.random.fold_in(rng, 6), dim), (parts,), jnp.float32, least / len(shards), high / len(shards))
        return jnp.repeat(jnp.exp(heights), extent[dim] // parts).reshape((-1,) + (1,) * (len(extent) - dim - 1))

    factor_of = one(*shards[0])
    for cut in shards[1:]:
        factor_of = factor_of * one(*cut)
    return factor_of


def centred(own_key, extent, scale, reach, cuts=(), held_as=jnp.bfloat16):
    result = scale * jax.random.normal(own_key, extent, jnp.float32)
    if cuts:
        result = result * steps_of(own_key, extent, cuts, -0.22, 0.18)
    return jnp.clip(result, -reach, reach).astype(held_as)


def gaussian_with(key, shape, scale, most, shards, heavy, kind=jnp.bfloat16):
    drawn = scale * jax.random.normal(key, shape, jnp.float32)
    if shards:
        drawn = drawn * steps_of(key, shape, shards, -0.22, 0.18)
    return jnp.clip(spiked(drawn, jax.random.fold_in(key, 3), *heavy), -most, most).astype(kind)


def setup_inputs(seed: int = 0) -> dict:
    key_of = jax.random.split(jax.random.key(seed), 10)
    return {
        "query_rows": draw_query_rows(jax.random.fold_in(key_of[9], 71), 0),
        "key_rows": draw_key_rows(jax.random.fold_in(key_of[9], 71), 0),
        "value_rows": centred(key_of[2], (TOKENS, HEADS * HEAD_DIM), 2.0, 12.0, ((0, 16), (1, 2))),
        "action_mask": draw_action_mask(jax.random.fold_in(key_of[9], 71), 0),
        "residual": draw_residual(jax.random.fold_in(key_of[9], 71), 0),
        "out_weight": centred(key_of[5], (D, HEADS * HEAD_DIM), (HEADS * HEAD_DIM) ** -0.5, 0.078125, ((1, 2),)),
        "norm_gain": jnp.clip(1.0 + 0.18 * jax.random.normal(key_of[6], (D,), jnp.float32), 0.1, 1.9),
        "upstream": gaussian_with(key_of[7], (TOKENS, D), 1.0, 6.0, ((0, 16), (1, 2)), (0, 1, 16, 2.0)),
        "residual_grad": centred(key_of[8], (TOKENS, D), 0.3, 2.0, ((0, 16), (1, 2))),
    }


epsilon = 1e-05

def visible(mask_row):
    position = jnp.arange(mask_row.shape[0])
    causal = position[None, :] <= position[:, None]
    observe = mask_row == 0
    return causal | observe[:, None] & observe[None, :]

def softmax_rows(query_heads, keyset, allowed):
    scores = jnp.einsum('qhd,khd->hqk', query_heads.astype(jnp.float32), keyset.astype(jnp.float32)) * HEAD_DIM ** (-0.5)
    masked = jnp.where(allowed[None], scores, -jnp.inf)
    row_top = lax.optimization_barrier(jnp.max(masked, axis=-1, keepdims=True))
    weights = jnp.exp(masked - row_top)
    return weights / lax.optimization_barrier(jnp.sum(weights, axis=-1, keepdims=True))

def split_heads(rows):
    return rows.reshape(LEN, HEADS, HEAD_DIM)

def forward_seq(inputs):
    query_seq, key_seq, value_seq, mask_row = inputs
    chances = softmax_rows(split_heads(query_seq), split_heads(key_seq), visible(mask_row))
    chances_low = lax.optimization_barrier(chances.astype(jnp.bfloat16)).astype(jnp.float32)
    attended = jnp.einsum('hqk,khd->qhd', chances_low, split_heads(value_seq).astype(jnp.float32))
    return attended.astype(jnp.bfloat16).reshape(LEN, HEADS * HEAD_DIM)

def backward_seq(inputs):
    query_seq, key_seq, value_seq, mask_row, grad_seq = inputs
    query_heads = split_heads(query_seq)
    key_heads = split_heads(key_seq)
    chances = softmax_rows(query_heads, key_heads, visible(mask_row))
    chances_low = lax.optimization_barrier(chances.astype(jnp.bfloat16)).astype(jnp.float32)
    grad_heads = split_heads(grad_seq).astype(jnp.float32)
    grad_value = jnp.einsum('hqk,qhd->khd', chances_low, grad_heads).astype(jnp.bfloat16)
    grad_chances = jnp.einsum('qhd,khd->hqk', grad_heads, split_heads(value_seq).astype(jnp.float32))
    row_delta = lax.optimization_barrier(jnp.sum(chances * grad_chances, axis=-1, keepdims=True))
    grad_scores = (chances * (grad_chances - row_delta) * HEAD_DIM ** (-0.5)).astype(jnp.bfloat16)
    grad_scores = lax.optimization_barrier(grad_scores).astype(jnp.float32)
    grad_query = jnp.einsum('hqk,khd->qhd', grad_scores, key_heads.astype(jnp.float32)).astype(jnp.bfloat16)
    grad_key = jnp.einsum('hqk,qhd->khd', grad_scores, query_heads.astype(jnp.float32)).astype(jnp.bfloat16)
    width = HEADS * HEAD_DIM
    return (grad_query.reshape(LEN, width), grad_key.reshape(LEN, width), grad_value.reshape(LEN, width))

def reference(query_rows, key_rows, value_rows, action_mask, residual, out_weight, norm_gain, upstream, residual_grad):
    width = HEADS * HEAD_DIM
    query_seq = query_rows.reshape(SEQS, LEN, width)
    key_seq = key_rows.reshape(SEQS, LEN, width)
    value_seq = value_rows.reshape(SEQS, LEN, width)
    attended = lax.map(forward_seq, (query_seq, key_seq, value_seq, action_mask)).reshape(TOKENS, width)
    projected = jnp.dot(attended, out_weight.T, preferred_element_type=jnp.float32)
    layer_out = (projected + residual.astype(jnp.float32)).astype(jnp.bfloat16)
    out_float = layer_out.astype(jnp.float32)
    row_rms = jnp.sqrt(lax.optimization_barrier(jnp.mean(out_float * out_float, axis=1, keepdims=True)) + epsilon)
    normed = out_float / row_rms
    scaled = upstream.astype(jnp.float32) * norm_gain[None, :]
    row_inner = lax.optimization_barrier(jnp.sum(scaled * out_float, axis=1, keepdims=True)) / (row_rms * D)
    grad_residual = (residual_grad.astype(jnp.float32) + (scaled - normed * row_inner) / row_rms).astype(jnp.bfloat16)
    grad_gain = lax.optimization_barrier(jnp.sum(upstream.astype(jnp.float32) * normed, axis=0))
    grad_out_weight = lax.dot_general(grad_residual, attended, (((0,), (0,)), ((), ())), preferred_element_type=jnp.float32)
    grad_attended = jnp.dot(grad_residual, out_weight, preferred_element_type=jnp.float32).astype(jnp.bfloat16)
    grad_seq = grad_attended.reshape(SEQS, LEN, width)
    grad_query, grad_key, grad_value = lax.map(backward_seq, (query_seq, key_seq, value_seq, action_mask, grad_seq))
    return (layer_out, grad_residual, grad_query.reshape(TOKENS, width), grad_key.reshape(TOKENS, width), grad_value.reshape(TOKENS, width), grad_out_weight, grad_gain)
```

```python
import functools

import jax
import jax.numpy as jnp
from jax import lax
from jax.experimental import pallas as pl
from jax.experimental.pallas import tpu as pltpu
from jax.sharding import PartitionSpec as P

HEAD_DIM = 128
LEN = 384

epsilon = 1e-05
SCALE = HEAD_DIM ** (-0.5)
NT = (((1,), (1,)), ((), ()))
TN = (((0,), (0,)), ((), ()))


def dot(a, b, dims):
    return lax.dot_general(a, b, dims, preferred_element_type=jnp.float32)


def forward_kernel(heads, observed_ref, query_ref, key_ref, value_ref, probs_ref, attended_ref):
    observed = observed_ref[pl.program_id(0)]
    row = lax.broadcasted_iota(jnp.int32, (LEN, LEN), 0)
    column = lax.broadcasted_iota(jnp.int32, (LEN, LEN), 1)
    allowed = column <= jnp.maximum(row, observed - 1)
    for head in range(heads):
        span = slice(head * HEAD_DIM, (head + 1) * HEAD_DIM)
        scores = dot(query_ref[:, span], key_ref[:, span], NT) * SCALE
        masked = jnp.where(allowed, scores, -jnp.inf)
        weights = jnp.exp(masked - jnp.max(masked, axis=1, keepdims=True))
        probs = weights * (1.0 / jnp.sum(weights, axis=1, keepdims=True))
        low = probs.astype(jnp.bfloat16)
        probs_ref[head] = low
        attended_ref[:, span] = jnp.dot(
            low, value_ref[:, span], preferred_element_type=jnp.float32
        ).astype(jnp.bfloat16)


def backward_kernel(
    heads, probs_ref, query_ref, key_ref, value_ref, cotangent_ref, query_out, key_out, value_out
):
    for head in range(heads):
        span = slice(head * HEAD_DIM, (head + 1) * HEAD_DIM)
        low = probs_ref[head]
        cotangent = cotangent_ref[:, span]
        value_out[:, span] = dot(low, cotangent, TN).astype(jnp.bfloat16)
        grad_probs = dot(cotangent, value_ref[:, span], NT)
        probs = low.astype(jnp.float32)
        delta = jnp.sum(probs * grad_probs, axis=1, keepdims=True)
        grad_scores = (probs * (grad_probs - delta) * SCALE).astype(jnp.bfloat16)
        query_out[:, span] = jnp.dot(
            grad_scores, key_ref[:, span], preferred_element_type=jnp.float32
        ).astype(jnp.bfloat16)
        key_out[:, span] = dot(grad_scores, query_ref[:, span], TN).astype(jnp.bfloat16)


def head_group(head_count):
    return max(size for size in range(1, 6) if head_count % size == 0)


def specs(heads):
    rows = pl.BlockSpec((LEN, heads * HEAD_DIM), lambda s, h: (s, h))
    square = pl.BlockSpec((None, heads, LEN, LEN), lambda s, h: (s, h, 0, 0))
    return rows, square


def attend(observed, query_rows, key_rows, value_rows):
    tok_rows, width = query_rows.shape
    head_count, seq_count = width // HEAD_DIM, tok_rows // LEN
    heads = head_group(head_count)
    rows, square = specs(heads)
    pairs = seq_count * head_count * LEN * LEN
    return pl.pallas_call(
        functools.partial(forward_kernel, heads),
        grid=(seq_count, head_count // heads),
        in_specs=[pl.BlockSpec(memory_space=pltpu.SMEM), rows, rows, rows],
        out_specs=[square, rows],
        out_shape=[
            jax.ShapeDtypeStruct((seq_count, head_count, LEN, LEN), jnp.bfloat16),
            jax.ShapeDtypeStruct((tok_rows, width), jnp.bfloat16),
        ],
        cost_estimate=pl.CostEstimate(
            flops=4 * pairs * HEAD_DIM,
            bytes_accessed=2 * pairs + 8 * tok_rows * width,
            transcendentals=pairs,
        ),
        name="attend",
    )(observed, query_rows, key_rows, value_rows)


def attend_backward(probs, query_rows, key_rows, value_rows, cotangent):
    tok_rows, width = query_rows.shape
    head_count, seq_count = width // HEAD_DIM, tok_rows // LEN
    heads = head_group(head_count)
    rows, square = specs(heads)
    pairs = seq_count * head_count * LEN * LEN
    return pl.pallas_call(
        functools.partial(backward_kernel, heads),
        grid=(seq_count, head_count // heads),
        in_specs=[square, rows, rows, rows, rows],
        out_specs=[rows, rows, rows],
        out_shape=[jax.ShapeDtypeStruct((tok_rows, width), jnp.bfloat16)] * 3,
        cost_estimate=pl.CostEstimate(
            flops=8 * pairs * HEAD_DIM,
            bytes_accessed=2 * pairs + 14 * tok_rows * width,
            transcendentals=0,
        ),
        name="attend_backward",
    )(probs, query_rows, key_rows, value_rows, cotangent)


def sum_groups(groups, value):
    if groups & (groups - 1):
        return lax.psum(value, "dp")
    bit = 1
    while bit < groups:
        value = value + lax.ppermute(value, "dp", [(i, i ^ bit) for i in range(groups)])
        bit *= 2
    return value


def shards(
    groups,
    tensor_size,
    query_rows,
    key_rows,
    value_rows,
    action_mask,
    residual,
    out_weight,
    norm_gain,
    upstream,
    residual_grad,
):
    model_width = out_weight.shape[0]
    own_width = residual.shape[1]
    pair = tensor_size == 2
    swap = [(0, 1), (1, 0)]
    mine = lax.axis_index("tensor")

    def weight_rows(index):
        return lax.dynamic_slice_in_dim(out_weight, index * own_width, own_width, 0)

    def sum_pair(value):
        if pair:
            return value + lax.ppermute(value, "tensor", swap)
        return lax.psum(value, "tensor")

    observed = jnp.sum((action_mask == 0).astype(jnp.int32), axis=1)
    probs, attended = attend(observed, query_rows, key_rows, value_rows)
    attended_all = lax.all_gather(attended, "dp", axis=0, tiled=True)
    if pair:
        theirs = dot(attended, weight_rows(1 - mine), NT).astype(jnp.bfloat16)
        arriving = lax.ppermute(theirs, "tensor", swap)
        own = dot(attended, weight_rows(mine), NT)
        own_sum = own + arriving.astype(jnp.float32)
    else:
        own_sum = lax.psum_scatter(
            dot(attended, out_weight, NT), "tensor", scatter_dimension=1, tiled=True
        )
    layer_out = (own_sum + residual.astype(jnp.float32)).astype(jnp.bfloat16)
    out_float = layer_out.astype(jnp.float32)
    upstream_float = upstream.astype(jnp.float32)
    scaled = upstream_float * norm_gain[None, :]
    sums = sum_pair(
        jnp.stack([jnp.sum(out_float * out_float, axis=1), jnp.sum(scaled * out_float, axis=1)])
    )
    row_rms = jnp.sqrt(sums[0] / model_width + epsilon)[:, None]
    normed = out_float / row_rms
    row_inner = sums[1][:, None] / (row_rms * model_width)
    grad_residual = (
        residual_grad.astype(jnp.float32) + (scaled - normed * row_inner) / row_rms
    ).astype(jnp.bfloat16)
    if pair:
        other = lax.ppermute(grad_residual, "tensor", swap)
        first = mine == 0
        low_half = jnp.where(first, grad_residual, other)
        high_half = jnp.where(first, other, grad_residual)
        grad_full = jnp.concatenate([low_half, high_half], axis=1)
        grad_attended = jnp.dot(
            grad_residual, weight_rows(mine), preferred_element_type=jnp.float32
        ) + jnp.dot(other, weight_rows(1 - mine), preferred_element_type=jnp.float32)
    else:
        grad_full = lax.all_gather(grad_residual, "tensor", axis=1, tiled=True)
        grad_attended = jnp.dot(grad_full, out_weight, preferred_element_type=jnp.float32)
    grad_attended = grad_attended.astype(jnp.bfloat16)
    received = lax.all_to_all(grad_full, "dp", split_axis=1, concat_axis=0, tiled=True)
    gain_part = jnp.sum(upstream_float * normed, axis=0)
    grad_query, grad_key, grad_value = attend_backward(
        probs, query_rows, key_rows, value_rows, grad_attended
    )
    grad_query, gain_part = lax.optimization_barrier((grad_query, gain_part))
    grad_gain = sum_groups(groups, gain_part)
    grad_out_weight = dot(received, attended_all, TN)
    return layer_out, grad_residual, grad_query, grad_key, grad_value, grad_out_weight, grad_gain


def solution(mesh):
    rows = P("dp", "tensor")
    return jax.shard_map(
        functools.partial(shards, mesh.shape["dp"], mesh.shape["tensor"]),
        mesh=mesh,
        in_specs=(
            rows,
            rows,
            rows,
            P("dp", None),
            rows,
            P(None, "tensor"),
            P("tensor"),
            rows,
            rows,
        ),
        out_specs=(rows, rows, rows, rows, rows, rows, P("tensor")),
        check_vma=False,
    )
```
